32 devices in a mesh: rep: 8 (over y, x, core), tp: 4 (over z).
Axes of the slice: x: 2, y: 2, z: 4, core: 2. Of those that a mesh axis runs over, the one named last changes fastest.
Arguments:
- tokens: bfloat16 [8192, 1280], P(('rep', 'tp')), may hold values from -6 to 6
- view_ids: int32 [32, 4], P('rep'), may hold values from 0 to 31
- time_ids: int32 [32], P('rep'), may hold values from 0 to 999
- camera_table: float32 [32, 1280], replicated, may hold values from -6 to 6
- norm_attn: float32 [2, 1280], replicated, may hold values from 0.1 to 1.9
- norm_ffn: float32 [2, 1280], replicated, may hold values from 0.1 to 1.9
- w_query: bfloat16 [2, 1280, 1280], P(None, ('rep', 'tp')), may hold values from -0.1677051 to 0.1677051
- w_key: bfloat16 [2, 1280, 1280], P(None, ('rep', 'tp')), may hold values from -6.764106 to 6.764106
- w_value: bfloat16 [2, 1280, 1280], P(None, ('rep', 'tp')), may hold values from -0.15625 to 0.15625
- w_out: bfloat16 [2, 1280, 1280], P(None, ('rep', 'tp')), may hold values from -0.15625 to 0.15625
- w_gate: bfloat16 [2, 1280, 5120], P(None, ('rep', 'tp')), may hold values from -0.15625 to 0.15625
- w_up: bfloat16 [2, 1280, 5120], P(None, ('rep', 'tp')), may hold values from -0.15625 to 0.15625
- w_down: bfloat16 [2, 1280, 5120], P(None, ('rep', 'tp')), may hold values from -0.078125 to 0.078125
Outputs:
- denoised: bfloat16 [8192, 1280], P(('rep', 'tp'))
The draws below stay inside these ranges and needn't reach their ends.
All inputs are finite; a program needn't handle non-finite values.
Results may differ from the reference program's by a relative error of at most 0.035.
Values may be sent and summed in bfloat16 or wider, within the bound.
No kernel may reach another device: no remote copies, remote signals or barrier semaphores. Data moves between devices by JAX's collectives and lax.ppermute only.
A program may use at most 128 MiB of HBM per device.

```python
import math
import jax
import jax.numpy as jnp
from jax import lax

D = 1280
FF = 5120
HEADS = 8
VIEWS = 4
HW = 64
LAYERS = 2
NPOSE = 32
CAMS = 32
ROWS = 8192
N_TP = 4


def query_base(key):
    base = jax.random.normal(jax.random.fold_in(key, 11), (LAYERS, D, D), jnp.float32)
    return jnp.clip(base, -6.0, 6.0) * D ** (-0.5)


def draw_w_query(key, part):
    return query_base(key).astype(jnp.bfloat16)


def draw_w_key(key, part):
    other = jax.random.normal(jax.random.fold_in(key, 12), (LAYERS, D, D), jnp.float32)
    other = jnp.clip(other, -6.0, 6.0) * D ** (-0.5)
    return other.astype(jnp.bfloat16)


def touch_ends(drawn, own_key, low, high):
    dims = drawn.shape
    spot = [jax.random.randint(jax.random.fold_in(own_key, axis), (), 0, dims[axis]) for axis in range(len(dims))]
    drawn = drawn.at[tuple(spot)].set(low)
    longest = dims.index(max(dims))
    spot[longest] = (spot[longest] + 1) % dims[longest]
    return drawn.at[tuple(spot)].set(high)


def block_scale(rng, dims, shards, smallest, top_value):
    loudness = 1.0
    for dim, parts in shards:
        draws = jax.random.uniform(jax.random.fold_in(jax.random.fold_in(rng, 6), dim), (parts,), jnp.float32, smallest / len(shards), top_value / len(shards))
        loudness = loudness * jnp.repeat(jnp.exp(draws), dims[dim] // parts).reshape((-1,) + (1,) * (len(dims) - 1 - dim))
    return loudness


def gaussian(key, shape, scale, limit, shards=(), kind=jnp.bfloat16):
    values = jax.random.normal(key, shape, jnp.float32) * scale
    if len(shards) > 0:
        values = block_scale(key, shape, shards, -0.22, 0.18) * values
    return jnp.clip(values, min=-limit, max=limit).astype(kind)


def setup_inputs(seed: int = 0) -> dict:
    streams_of = jax.random.split(jax.random.key(seed), 14)
    tokens = gaussian(streams_of[0], (ROWS, D), 1.0, 6.0, ((0, 32),))
    view_ids = touch_ends(jax.random.randint(streams_of[1], (CAMS, VIEWS), 0, NPOSE), jax.random.fold_in(streams_of[1], 1), 0, NPOSE - 1).astype(jnp.int32)
    time_ids = touch_ends(jax.random.randint(streams_of[2], (CAMS,), 0, 1000), jax.random.fold_in(streams_of[2], 1), 0, 999).astype(jnp.int32)
    camera_table = gaussian(streams_of[3], (NPOSE, D), 1.0, 6.0, (), jnp.float32)
    norm_attn = jnp.clip(1.0 + 0.18 * jax.random.normal(streams_of[4], (LAYERS, D), jnp.float32), 0.1, 1.9)
    norm_ffn = jnp.clip(1.0 + 0.18 * jax.random.normal(streams_of[5], (LAYERS, D), jnp.float32), 0.1, 1.9)
    w_query = draw_w_query(jax.random.fold_in(streams_of[13], 71), 0)
    w_key = draw_w_key(jax.random.fold_in(streams_of[13], 71), 0)
    w_value = gaussian(streams_of[8], (LAYERS, D, D), D ** -0.5, 0.15625, ((1, 32),))
    w_out = gaussian(streams_of[9], (LAYERS, D, D), D ** -0.5, 0.15625, ((1, 32),))
    w_gate = gaussian(streams_of[10], (LAYERS, D, FF), D ** -0.5, 0.15625, ((1, 32),))
    w_up = gaussian(streams_of[11], (LAYERS, D, FF), D ** -0.5, 0.15625, ((1, 32),))
    w_down = gaussian(streams_of[12], (LAYERS, D, FF), FF ** -0.5, 0.078125, ((1, 32),))
    return dict(tokens=tokens, view_ids=view_ids, time_ids=time_ids, camera_table=camera_table, norm_attn=norm_attn, norm_ffn=norm_ffn, w_query=w_query, w_key=w_key, w_value=w_value, w_out=w_out, w_gate=w_gate, w_up=w_up, w_down=w_down)


def layer_norm(activations, gain_vector):
    average = lax.optimization_barrier(jnp.mean(activations, axis=-1, keepdims=True))
    centred = activations - average
    spread = lax.optimization_barrier(jnp.mean(centred * centred, axis=-1, keepdims=True))
    return (centred * lax.rsqrt(spread + 1e-05) * gain_vector).astype(jnp.bfloat16)

def time_code(step_ids, width):
    half_width = width // 2
    frequency = jnp.exp(-math.log(10000.0) * jnp.arange(half_width, dtype=jnp.float32) / half_width)
    angles = step_ids.astype(jnp.float32)[:, None] * frequency[None, :]
    return jnp.concatenate([jnp.cos(angles), jnp.sin(angles)], axis=1)

def split_sum(mixed_rows, weight):
    row_count = mixed_rows.shape[0]
    inner_width = mixed_rows.shape[1] // N_TP
    left_side = mixed_rows.astype(jnp.float32).reshape(row_count, N_TP, inner_width)
    right_side = weight.astype(jnp.float32).reshape(weight.shape[0], N_TP, inner_width)
    term_rows = jnp.einsum('snc,onc->nso', left_side, right_side).astype(jnp.bfloat16)
    term_rows = lax.optimization_barrier(term_rows)
    return lax.optimization_barrier(jnp.sum(term_rows.astype(jnp.float32), axis=0))

def attention(query_rows, key_rows, value_rows):
    seq_len = query_rows.shape[0]
    head_size = D // HEADS
    query_heads = query_rows.astype(jnp.float32).reshape(seq_len, HEADS, head_size)
    key_heads = key_rows.astype(jnp.float32).reshape(seq_len, HEADS, head_size)
    value_heads = value_rows.astype(jnp.float32).reshape(seq_len, HEADS, head_size)
    scores = jnp.einsum('qhd,khd->hqk', query_heads, key_heads) * head_size ** (-0.5)
    peak = lax.optimization_barrier(jnp.max(scores, axis=-1, keepdims=True))
    expons = jnp.exp(scores - peak)
    attn_probs = (expons / lax.optimization_barrier(jnp.sum(expons, axis=-1, keepdims=True))).astype(jnp.bfloat16)
    mixed_rows = jnp.einsum('hqk,khd->qhd', attn_probs.astype(jnp.float32), value_heads)
    return mixed_rows.astype(jnp.bfloat16).reshape(seq_len, D)

def reference(tokens, view_ids, time_ids, camera_table, norm_attn, norm_ffn, w_query, w_key, w_value, w_out, w_gate, w_up, w_down):
    seq_len = VIEWS * HW
    set_count = tokens.shape[0] // seq_len
    blocks = tokens.reshape(set_count, seq_len, D)

    def one_set(packed):
        block, views_here, step_here = packed
        camera = jnp.repeat(camera_table[views_here], HW, axis=0)
        stream = block.astype(jnp.float32) + camera + time_code(step_here[None], D)
        for layer_index in range(LAYERS):
            normed = layer_norm(stream, norm_attn[layer_index])
            query_rows = jnp.dot(normed, w_query[layer_index], preferred_element_type=jnp.float32).astype(jnp.bfloat16)
            key_rows = jnp.dot(normed, w_key[layer_index], preferred_element_type=jnp.float32).astype(jnp.bfloat16)
            value_rows = jnp.dot(normed, w_value[layer_index], preferred_element_type=jnp.float32).astype(jnp.bfloat16)
            mixed_rows = attention(query_rows, key_rows, value_rows)
            stream = stream + split_sum(mixed_rows, w_out[layer_index])
            normed = layer_norm(stream, norm_ffn[layer_index])
            gate_part = jnp.dot(normed, w_gate[layer_index], preferred_element_type=jnp.float32)
            up_part = jnp.dot(normed, w_up[layer_index], preferred_element_type=jnp.float32)
            hidden = (jax.nn.gelu(gate_part, approximate=False) * up_part).astype(jnp.bfloat16)
            stream = stream + split_sum(hidden, w_down[layer_index])
        return stream.astype(jnp.bfloat16)
    result = lax.map(one_set, (blocks, view_ids, time_ids))
    return result.reshape(tokens.shape[0], D)
```

```python
import math

import jax
import jax.numpy as jnp
from jax import lax
from jax.sharding import PartitionSpec as P

HEADS = 8
VIEWS = 4
HW = 64
PAIR = 2


def layer_norm(activations, gain_vector):
    average = jnp.mean(activations, axis=-1, keepdims=True)
    centred = activations - average
    spread = jnp.mean(centred * centred, axis=-1, keepdims=True)
    return (centred * lax.rsqrt(spread + 1e-05) * gain_vector).astype(jnp.bfloat16)


def time_code(step_ids, width):
    half_width = width // 2
    frequency = jnp.exp(-math.log(10000.0) * jnp.arange(half_width, dtype=jnp.float32) / half_width)
    angles = step_ids.astype(jnp.float32)[:, None] * frequency[None, :]
    return jnp.concatenate([jnp.cos(angles), jnp.sin(angles)], axis=1)


def conditioning(share_rows, view_ids, time_ids, camera_table):
    slot_count = share_rows // HW
    slot_ids = lax.axis_index("tp") * slot_count + jnp.arange(slot_count, dtype=jnp.int32)
    flat_views = view_ids.reshape(-1)
    slot_range = jnp.arange(flat_views.shape[0], dtype=jnp.int32)
    pose_ids = jnp.sum(
        jnp.where(slot_ids[:, None] == slot_range[None, :], flat_views[None, :], 0), axis=1
    )
    set_range = jnp.arange(time_ids.shape[0], dtype=jnp.int32)
    step_ids = jnp.sum(
        jnp.where((slot_ids // VIEWS)[:, None] == set_range[None, :], time_ids[None, :], 0), axis=1
    )
    pose_range = jnp.arange(camera_table.shape[0], dtype=jnp.int32)
    onehot_pose = (pose_ids[:, None] == pose_range[None, :]).astype(jnp.float32)
    camera = jnp.dot(onehot_pose, camera_table, precision=lax.Precision.HIGHEST)
    return camera + time_code(step_ids, camera_table.shape[1])


def exchange(value, step, count):
    return lax.ppermute(value, "tp", [(i, i ^ step) for i in range(count)])


def column_halves(shards):
    def pack(part):
        pieces = []
        for shard in shards:
            half = shard.shape[1] // PAIR
            pieces.append(shard[:, part * half : (part + 1) * half])
        return jnp.concatenate(pieces, axis=1)

    return pack(0), pack(1)


def gather_pack(shards, tp_index, tp_count):
    first, second = column_halves(shards)
    lower = tp_index % PAIR == 0
    mine = jnp.where(lower, first, second)
    other = jnp.where(lower, second, first)
    rows, columns = mine.shape
    stacked = jnp.zeros((tp_count, rows, columns), mine.dtype)
    stacked = lax.dynamic_update_slice(stacked, mine[None], (tp_index, 0, 0))
    for step in range(1, tp_count):
        arrived = exchange(mine if step % PAIR == 0 else other, step, tp_count)
        stacked = lax.dynamic_update_slice(stacked, arrived[None], (tp_index ^ step, 0, 0))
    return lax.all_gather(stacked.reshape(tp_count * rows, columns), "rep", axis=0, tiled=True)


def attend(packed, head_count, head_size):
    total_rows = packed.shape[0]
    seq_len = VIEWS * HW
    width = head_count * head_size
    shape_heads = (total_rows // seq_len, seq_len, head_count, head_size)
    query_rows = packed[:, :width].reshape(shape_heads)
    key_rows = packed[:, width : 2 * width].reshape(shape_heads)
    value_rows = packed[:, 2 * width :].reshape(shape_heads)
    scores = jnp.einsum(
        "bqhd,bkhd->bhqk", query_rows, key_rows, preferred_element_type=jnp.float32
    ) * head_size ** (-0.5)
    peak = jnp.max(scores, axis=-1, keepdims=True)
    expons = jnp.exp(scores - peak)
    attn_probs = (expons / jnp.sum(expons, axis=-1, keepdims=True)).astype(jnp.bfloat16)
    mixed_rows = jnp.einsum(
        "bhqk,bkhd->bqhd", attn_probs, value_rows, preferred_element_type=jnp.float32
    )
    return mixed_rows.astype(jnp.bfloat16).reshape(total_rows, width)


def transposed_dot(left, right):
    return lax.dot_general(
        left, right, (((1,), (1,)), ((), ())), preferred_element_type=jnp.float32
    )


def body(
    tokens,
    view_ids,
    time_ids,
    camera_table,
    norm_attn,
    norm_ffn,
    w_query,
    w_key,
    w_value,
    w_out,
    w_gate,
    w_up,
    w_down,
):
    tp_count = lax.axis_size("tp")
    tp_index = lax.axis_index("tp")
    share_rows, channels = tokens.shape
    layers = w_query.shape[0]
    head_count = HEADS // PAIR
    head_size = channels // HEADS
    width = head_count * head_size
    inner = w_gate.shape[2] // PAIR

    attn_packs = []
    ffn_packs = []
    for layer in range(layers):
        attn_packs.append(
            gather_pack(
                [w_query[layer], w_key[layer], w_value[layer], w_out[layer]], tp_index, tp_count
            )
        )
        ffn_packs.append(
            gather_pack([w_gate[layer], w_up[layer], w_down[layer]], tp_index, tp_count)
        )

    slots = conditioning(share_rows, view_ids, time_ids, camera_table)
    stream = (
        tokens.astype(jnp.float32).reshape(-1, HW, channels) + slots[:, None, :]
    ).reshape(share_rows, channels)

    def pair_update(stream, partial_rows):
        arrived = exchange(partial_rows[share_rows:].astype(jnp.bfloat16), 1, tp_count)
        return stream + partial_rows[:share_rows] + arrived.astype(jnp.float32)

    for layer in range(layers):
        attn_w = attn_packs[layer]
        ffn_w = ffn_packs[layer]
        normed = layer_norm(stream, norm_attn[layer])
        rows = jnp.concatenate([normed, exchange(normed, 1, tp_count)], axis=0)
        packed = jnp.dot(
            rows, attn_w[:, : 3 * width], preferred_element_type=jnp.float32
        ).astype(jnp.bfloat16)
        mixed = attend(packed, head_count, head_size)
        stream = pair_update(stream, transposed_dot(mixed, attn_w[:, 3 * width :]))
        normed = layer_norm(stream, norm_ffn[layer])
        rows = jnp.concatenate([normed, exchange(normed, 1, tp_count)], axis=0)
        gate_part = jnp.dot(rows, ffn_w[:, :inner], preferred_element_type=jnp.float32)
        up_part = jnp.dot(rows, ffn_w[:, inner : 2 * inner], preferred_element_type=jnp.float32)
        hidden = (jax.nn.gelu(gate_part, approximate=False) * up_part).astype(jnp.bfloat16)
        hidden = lax.optimization_barrier(hidden)
        stream = pair_update(stream, transposed_dot(hidden, ffn_w[:, 2 * inner :]))
    return stream.astype(jnp.bfloat16)


def solution(mesh):
    return jax.shard_map(
        body,
        mesh=mesh,
        in_specs=(
            P(("rep", "tp"), None),
            P("rep", None),
            P("rep"),
            P(),
            P(),
            P(),
            P(None, ("rep", "tp"), None),
            P(None, ("rep", "tp"), None),
            P(None, ("rep", "tp"), None),
            P(None, ("rep", "tp"), None),
            P(None, ("rep", "tp"), None),
            P(None, ("rep", "tp"), None),
            P(None, ("rep", "tp"), None),
        ),
        out_specs=P(("rep", "tp"), None),
        check_vma=False,
    )
```

```python
import functools
import math

import jax
import jax.numpy as jnp
from jax import lax
from jax.experimental import pallas as pl
from jax.experimental.pallas import tpu as pltpu
from jax.sharding import PartitionSpec as P


HEADS = 8
VIEWS = 4
HW = 64
PAIR = 2


def layer_norm(activations, gain_vector):
    average = jnp.mean(activations, axis=-1, keepdims=True)
    centred = activations - average
    spread = jnp.mean(centred * centred, axis=-1, keepdims=True)
    return (centred * lax.rsqrt(spread + 1e-05) * gain_vector).astype(jnp.bfloat16)


def time_code(step_ids, width):
    half_width = width // 2
    frequency = jnp.exp(-math.log(10000.0) * jnp.arange(half_width, dtype=jnp.float32) / half_width)
    angles = step_ids.astype(jnp.float32)[:, None] * frequency[None, :]
    return jnp.concatenate([jnp.cos(angles), jnp.sin(angles)], axis=1)


def conditioning(share_rows, view_ids, time_ids, camera_table):
    slot_count = share_rows // HW
    slot_ids = lax.axis_index("tp") * slot_count + jnp.arange(slot_count, dtype=jnp.int32)
    flat_views = view_ids.reshape(-1)
    slot_range = jnp.arange(flat_views.shape[0], dtype=jnp.int32)
    pose_ids = jnp.sum(
        jnp.where(slot_ids[:, None] == slot_range[None, :], flat_views[None, :], 0), axis=1
    )
    set_range = jnp.arange(time_ids.shape[0], dtype=jnp.int32)
    step_ids = jnp.sum(
        jnp.where((slot_ids // VIEWS)[:, None] == set_range[None, :], time_ids[None, :], 0), axis=1
    )
    pose_range = jnp.arange(camera_table.shape[0], dtype=jnp.int32)
    onehot_pose = (pose_ids[:, None] == pose_range[None, :]).astype(jnp.float32)
    camera = jnp.dot(onehot_pose, camera_table, precision=lax.Precision.HIGHEST)
    return camera + time_code(step_ids, camera_table.shape[1])


def exchange(value, step):
    count = lax.axis_size("tp")
    return lax.ppermute(value, "tp", [(i, i ^ step) for i in range(count)])


def swap(value, mask):
    count = lax.axis_size("rep")
    return lax.ppermute(value, "rep", [(i, i ^ mask) for i in range(count)])


def pack_kernel(count, lower_ref, *refs):
    mine_ref, other_ref = refs[count:]
    lower = lower_ref[0] != 0
    start = 0
    for ref in refs[:count]:
        half = ref.shape[2] // PAIR
        first, second = ref[0, :, :half], ref[0, :, half:]
        mine_ref[:, start : start + half] = jnp.where(lower, first, second)
        other_ref[:, start : start + half] = jnp.where(lower, second, first)
        start += half


def column_halves(weights, layer, lower):
    rows = weights[0].shape[1]
    columns = sum(weight.shape[2] // PAIR for weight in weights)
    whole = pl.BlockSpec((rows, columns), lambda j, lower: (0, 0))
    return pl.pallas_call(
        functools.partial(pack_kernel, len(weights)),
        grid_spec=pltpu.PrefetchScalarGridSpec(
            num_scalar_prefetch=1,
            grid=(1,),
            in_specs=[
                pl.BlockSpec((1, *weight.shape[1:]), lambda j, lower: (layer, 0, 0))
                for weight in weights
            ],
            out_specs=[whole, whole],
        ),
        out_shape=[jax.ShapeDtypeStruct((rows, columns), weights[0].dtype)] * 2,
        compiler_params=pltpu.CompilerParams(vmem_limit_bytes=(24 if layer else 60) * 2**20),
        cost_estimate=pl.CostEstimate(
            flops=rows * columns, bytes_accessed=8 * rows * columns, transcendentals=0
        ),
        name="column_halves",
    )(lower.astype(jnp.int32).reshape(1), *weights)


def tp_steps(tp_count):
    return [step for step in range(1, tp_count) if step != 1] + [1]


def send_tp(shards, tp_index, tp_count, clock=None):
    weights, layer = shards
    mine, other = column_halves(weights, layer, tp_index % PAIR == 0)
    if clock is not None:
        mine, other = clock.take(mine, other)
    arrivals = [exchange(mine if step % PAIR == 0 else other, step) for step in tp_steps(tp_count)]
    return mine, arrivals


def join_tp(mine, arrivals, tp_index, tp_count):
    rows, columns = mine.shape
    stacked = jnp.broadcast_to(mine[None], (tp_count, rows, columns))
    for step, arrived in zip(tp_steps(tp_count), arrivals):
        stacked = lax.dynamic_update_slice(stacked, arrived[None], (tp_index ^ step, 0, 0))
    return stacked.reshape(tp_count * rows, columns)


def send_near(block):
    return swap(block, 2), swap(block, 4)


def send_far(near, far):
    half = near.shape[0] // 2
    return swap(near[:half], 4), swap(far[half:], 2)


def gather_rep(block):
    chips = lax.axis_size("rep") // 2
    pieces = [block]
    for bit in range(1, chips.bit_length()):
        pieces = pieces + [swap(piece, 1 << bit) for piece in pieces]
    own = jnp.concatenate(pieces, axis=0)
    return own, swap(own, 1)


class Clock:
    def __init__(self, channels):
        self.ones = jnp.ones((1, channels), jnp.float32)
        self.doubled = False
        self.token = self.ones

    def take(self, *values, name=None):
        if name is not None:
            self.ones = self.ones * (0.5 if self.doubled else 2.0)
            self.doubled = not self.doubled
        out = lax.optimization_barrier((*values, self.token, self.ones))
        self.ones = out[-1]
        self.token = out[0]
        return out[: len(values)] if len(values) > 1 else out[0]

    def one(self):
        return self.ones * (0.5 if self.doubled else 1.0)


def channel_order(channels):
    groups = lax.axis_size("rep")
    span = channels // groups
    place = jnp.arange(channels, dtype=jnp.int32)
    slot = place // span
    mask = 2 * (slot % (groups // 2)) + slot // (groups // 2)
    natural = (lax.axis_index("rep") ^ mask) * span + place % span
    return (jnp.arange(channels, dtype=jnp.int32)[:, None] == natural[None, :])


def transposed_dot(left, right):
    return lax.dot_general(left, right, (((1,), (1,)), ((), ())), preferred_element_type=jnp.float32)


def whole(refs):
    return jnp.concatenate([ref[...] for ref in refs], axis=0)


def ffn_kernel(count, rows_ref, *refs):
    gates, ups, downs = refs[:count], refs[count : 2 * count], refs[2 * count : 3 * count]
    out_ref, sum_ref = refs[3 * count], refs[3 * count + 1]
    step = pl.program_id(0)

    @pl.when(step == 0)
    def _():
        sum_ref[...] = jnp.zeros_like(sum_ref)

    rows = rows_ref[...]
    gate_part = jnp.dot(rows, whole(gates), preferred_element_type=jnp.float32)
    up_part = jnp.dot(rows, whole(ups), preferred_element_type=jnp.float32)
    gelu = 0.5 * gate_part * (1.0 + lax.erf(gate_part * (0.5**0.5)))
    hidden = (gelu * up_part).astype(jnp.bfloat16)
    sum_ref[...] += transposed_dot(hidden, whole(downs))

    @pl.when(step == pl.num_programs(0) - 1)
    def _():
        out_ref[...] = sum_ref[...].astype(out_ref.dtype)


def ffn_terms(rows, gate, up, down, inner, dtype):
    count = len(gate)
    block = next(size for size in (512, 256, 128) if inner % size == 0)
    steps = inner // block
    total, channels = rows.shape
    specs = [pl.BlockSpec((total, channels), lambda j: (0, 0))]
    shift = up[0].shape[1] // block - steps
    specs += [pl.BlockSpec((piece.shape[0], block), lambda j: (0, j)) for piece in gate]
    specs += [pl.BlockSpec((piece.shape[0], block), lambda j: (0, j + shift)) for piece in up]
    specs += [pl.BlockSpec((piece.shape[0], block), lambda j: (0, j)) for piece in down]
    return pl.pallas_call(
        functools.partial(ffn_kernel, count),
        grid=(steps,),
        in_specs=specs,
        out_specs=pl.BlockSpec((total, channels), lambda j: (0, 0)),
        out_shape=jax.ShapeDtypeStruct((total, channels), dtype),
        scratch_shapes=[pltpu.VMEM((total, channels), jnp.float32)],
        compiler_params=pltpu.CompilerParams(
            dimension_semantics=("arbitrary",), vmem_limit_bytes=28 * 2**20
        ),
        cost_estimate=pl.CostEstimate(
            flops=6 * total * channels * inner, bytes_accessed=6 * channels * inner, transcendentals=0
        ),
        name="ffn_terms",
    )(rows, *gate, *up, *down)


def attention_kernel(count, heads, size, rows_ref, *refs):
    weights, out_ref = refs[:count], refs[count]
    mixed_ref = refs[count + 1]
    width = heads * size
    weight = whole(weights)
    packed = jnp.dot(rows_ref[...], weight[:, : 3 * width], preferred_element_type=jnp.float32)
    packed = packed.astype(jnp.bfloat16)
    mixed_ref[...] = jnp.zeros_like(mixed_ref)
    for head in range(heads):
        low, high = head * size, (head + 1) * size
        left = low // 128 * 128
        right = min(-(-high // 128) * 128, width)
        lane = lax.broadcasted_iota(jnp.int32, (1, right - left), 1) + left
        here = (lane >= low) & (lane < high)
        query = jnp.where(here, packed[:, left:right], 0)
        key = packed[:, width + left : width + right]
        value = packed[:, 2 * width + left : 2 * width + right]
        scores = transposed_dot(query, key) * size ** (-0.5)
        peak = jnp.max(scores, axis=-1, keepdims=True)
        expons = jnp.exp(scores - peak)
        probs = (expons / jnp.sum(expons, axis=-1, keepdims=True)).astype(jnp.bfloat16)
        mixed = jnp.dot(probs, value, preferred_element_type=jnp.float32)
        mixed_ref[:, left:right] += jnp.where(here, mixed, 0.0)
    mixed = mixed_ref[...].astype(jnp.bfloat16)
    out_ref[...] = transposed_dot(mixed, weight[:, 3 * width :]).astype(out_ref.dtype)


def attention_terms(rows, weights, heads, size, seq_len, dtype):
    total, channels = rows.shape
    width = heads * size
    specs = [pl.BlockSpec((seq_len, channels), lambda j: (j, 0))]
    specs += [pl.BlockSpec(piece.shape, lambda j: (0, 0)) for piece in weights]
    return pl.pallas_call(
        functools.partial(attention_kernel, len(weights), heads, size),
        grid=(total // seq_len,),
        in_specs=specs,
        out_specs=pl.BlockSpec((seq_len, channels), lambda j: (j, 0)),
        out_shape=jax.ShapeDtypeStruct((total, channels), dtype),
        scratch_shapes=[pltpu.VMEM((seq_len, width), jnp.float32)],
        compiler_params=pltpu.CompilerParams(
            dimension_semantics=("arbitrary",), vmem_limit_bytes=28 * 2**20
        ),
        cost_estimate=pl.CostEstimate(
            flops=2 * total * (4 * channels + 2 * seq_len) * width,
            bytes_accessed=8 * channels * width,
            transcendentals=0,
        ),
        name="attention_terms",
    )(rows, *weights)


def run_plain(stream, shards, gains_attn, gains_ffn, attn, ffn, tp_index, tp_count):
    packs = {}
    for name, parts in shards.items():
        sent = send_tp(parts, tp_index, tp_count)
        packs[name] = gather_rep(join_tp(*sent, tp_index, tp_count))
    share_rows = stream.shape[0]

    def half_layer(stream, gain, terms):
        normed = layer_norm(stream, gain)
        peer = exchange(normed, 1)
        both = terms(jnp.concatenate([normed, peer], axis=0))
        arrived = exchange(both[share_rows:].astype(jnp.bfloat16), 1)
        return stream + both[:share_rows] + arrived.astype(jnp.float32)

    for layer in range(gains_attn.shape[0]):
        attn_w, down_w = packs[f"A{layer}"], packs[f"N{layer}"]
        gate_w = packs["P0" if layer == 0 else f"G{layer}"]
        up_w = packs["U0" if layer == 0 else f"G{layer}"]
        stream = half_layer(stream, gains_attn[layer], lambda rows: attn(rows, attn_w, jnp.float32))
        stream = half_layer(
            stream, gains_ffn[layer], lambda rows: ffn(rows, gate_w, up_w, down_w, jnp.float32)
        )
    return stream


def run_ordered(stream, shards, gains_attn, gains_ffn, attn, ffn, tp_index, tp_count):
    clock = Clock(stream.shape[1])
    block, near, diag, early, late, sent = ({} for _ in range(6))

    def send(name, ordered=False):
        sent[name] = send_tp(shards[name], tp_index, tp_count, clock if ordered else None)

    def take_z(name):
        mine, arrivals = sent[name]
        block[name] = join_tp(mine, clock.take(*arrivals, name="Z" + name), tp_index, tp_count)
        near[name] = send_near(block[name])
        early[name] = [swap(block[name], 1)]

    def take_d(name):
        near[name] = clock.take(*near[name], name="D" + name)
        diag[name] = send_far(*near[name])
        early[name] += [swap(near[name][0], 1), swap(near[name][1], 1)]

    def take_f(name):
        taken = clock.take(*diag[name], *early[name], name="F" + name)
        diag[name], early[name] = taken[:2], list(taken[2:])
        late[name] = [swap(diag[name][0], 1), swap(diag[name][1], 1)]

    def take_c(peer, *names):
        late_pieces = [piece for name in names for piece in late[name]]
        taken = clock.take(peer, *late_pieces, name="C" + names[0])
        for place, name in enumerate(names):
            late[name] = list(taken[1 + 2 * place : 3 + 2 * place])
        return taken[0]

    def weight(name):
        return [block[name], *near[name], *diag[name], *early[name], *late[name]]

    def begin(stream, gain):
        normed = layer_norm(stream, gain)
        return normed, exchange(normed, 1)

    def attn_peer(peer, name):
        peer = take_c(peer, name)
        return exchange(clock.take(attn(peer, weight(name), jnp.bfloat16)), 1)

    def attn_own(normed, name):
        return attn(clock.take(normed), weight(name), jnp.float32)

    def ffn_peer(peer, names):
        peer = take_c(peer, *names)
        terms = ffn(peer, weight(names[0]), weight(names[-2]), weight(names[-1]), jnp.bfloat16)
        return exchange(clock.take(terms), 1)

    def ffn_own(normed, names):
        normed = clock.take(normed)
        return ffn(normed, weight(names[0]), weight(names[-2]), weight(names[-1]), jnp.float32)

    def finish(stream, own_terms, arrived, name=None):
        return stream + own_terms + clock.take(arrived, name=name).astype(jnp.float32)

    first, second = ("P0", "U0", "N0"), ("G1", "N1")
    send("A0")
    normed, peer = begin(stream, gains_attn[0])
    normed = clock.take(normed)
    for name in first:
        send(name, True)
    for name in ("A1", *second):
        send(name)
    take_z("A0")
    take_d("A0")
    take_z("P0")
    take_f("A0")
    arrived = attn_peer(peer, "A0")
    own_terms = attn_own(normed, "A0")
    take_z("U0")
    take_d("P0")
    stream = finish(stream, own_terms, arrived, "X1")
    normed, peer = begin(stream, gains_ffn[0])
    take_z("N0")
    take_d("U0")
    take_f("P0")
    take_d("N0")
    take_z("A1")
    take_f("U0")
    take_f("N0")
    arrived = ffn_peer(peer, first)
    take_d("A1")
    take_z("G1")
    own_terms = ffn_own(normed, first)
    take_f("A1")
    stream = finish(stream, own_terms, arrived, "X3")
    normed, peer = begin(stream, gains_attn[1])
    take_z("N1")
    arrived = attn_peer(peer, "A1")
    own_terms = attn_own(normed, "A1")
    take_d("G1")
    stream = finish(stream, own_terms, arrived, "X5")
    normed, peer = begin(stream, gains_ffn[1])
    take_d("N1")
    take_f("G1")
    take_f("N1")
    arrived = ffn_peer(peer, second)
    own_terms = ffn_own(normed, second)
    return finish(stream, own_terms, arrived) * clock.one()


def body(
    tokens,
    view_ids,
    time_ids,
    camera_table,
    norm_attn,
    norm_ffn,
    w_query,
    w_key,
    w_value,
    w_out,
    w_gate,
    w_up,
    w_down,
):
    tp_count = lax.axis_size("tp")
    tp_index = lax.axis_index("tp")
    share_rows, channels = tokens.shape
    layers = w_query.shape[0]
    head_count = HEADS // PAIR
    head_size = channels // HEADS
    inner = w_gate.shape[2] // PAIR

    order = channel_order(channels)
    slots = conditioning(share_rows, view_ids, time_ids, camera_table)
    small = jnp.concatenate([norm_attn, norm_ffn, slots], axis=0)
    small = jnp.dot(small, order.astype(jnp.float32), precision=lax.Precision.HIGHEST)
    gains_attn = small[:layers]
    gains_ffn = small[layers : 2 * layers]
    slots = small[2 * layers :]
    stream = jnp.dot(tokens, order.astype(jnp.bfloat16), preferred_element_type=jnp.float32)
    stream = (stream.reshape(-1, HW, channels) + slots[:, None, :]).reshape(share_rows, channels)

    seq_len = VIEWS * HW
    shards = {}
    for layer in range(layers):
        shards[f"A{layer}"] = [w_query, w_key, w_value, w_out], layer
        if layer == 0:
            shards["P0"] = [w_gate], layer
            shards["U0"] = [w_up], layer
        else:
            shards[f"G{layer}"] = [w_gate, w_up], layer
        shards[f"N{layer}"] = [w_down], layer

    def attn(rows, weight, dtype):
        return attention_terms(rows, weight, head_count, head_size, seq_len, dtype)

    def ffn(rows, gate_w, up_w, down_w, dtype):
        return ffn_terms(rows, gate_w, up_w, down_w, inner, dtype)

    if share_rows % seq_len == 0 and layers == 2 and lax.axis_size("rep") == 8:
        stream = run_ordered(stream, shards, gains_attn, gains_ffn, attn, ffn, tp_index, tp_count)
    else:
        stream = run_plain(stream, shards, gains_attn, gains_ffn, attn, ffn, tp_index, tp_count)
    result = stream.astype(jnp.bfloat16)
    return lax.dot_general(
        result,
        order.astype(jnp.bfloat16),
        (((1,), (1,)), ((), ())),
        preferred_element_type=jnp.float32,
    ).astype(jnp.bfloat16)


def solution(mesh):
    return jax.shard_map(
        body,
        mesh=mesh,
        in_specs=(
            P(("rep", "tp"), None),
            P("rep", None),
            P("rep"),
            P(),
            P(),
            P(),
            P(None, ("rep", "tp"), None),
            P(None, ("rep", "tp"), None),
            P(None, ("rep", "tp"), None),
            P(None, ("rep", "tp"), None),
            P(None, ("rep", "tp"), None),
            P(None, ("rep", "tp"), None),
            P(None, ("rep", "tp"), None),
        ),
        out_specs=P(("rep", "tp"), None),
        check_vma=False,
    )
```
